8 devices in a mesh: data: 2 (over z, y), seq: 4 (over x, core).
Axes of the slice: x: 2, y: 2, z: 1, core: 2. Of those that a mesh axis runs over, the one named last changes fastest.
Arguments:
- x_in: bfloat16 [4096, 4096], P(('data', 'seq')), parts along dimension 0
- g_attn: float32 [4096], replicated
- w_qkv: bfloat16 [4096, 12288], replicated
- w_out: bfloat16 [16, 256, 4096], replicated
- g_mlp: float32 [4096], replicated
- w_gate: bfloat16 [4096, 16384], replicated
- w_up: bfloat16 [4096, 16384], replicated
- w_down: bfloat16 [16384, 4096], replicated
Outputs:
- output: bfloat16 [4096, 4096], P(('data', 'seq')), parts along dimension 0
There are 2 independent parts. The reference program is written for one: setup_inputs(seed, part) draws one part's arguments, and reference() takes and returns one part's arrays. A program takes and returns all parts, laid end to end along the dimension named above; an argument that names none is the same for every part.
All inputs are finite; a program needn't handle non-finite values.
Results may differ from the reference program's by a relative error of at most 0.00758202.
Values are sent between devices in bfloat16 or wider.
A program may use at most 2.25 GiB of HBM per device.

```python
import jax
import jax.numpy as jnp
from jax import lax

SEQ_LEN = 2048
BLOCK_ROWS = 512
D = 4096
HEADS = 16
HEAD = 256
FF = 16384
ROPE_BASE = 10000
WALK_RANK = 8


def setup_inputs(seed: int = 0, part: int = 0) -> dict:
    part_key = jax.random.fold_in(jax.random.key(seed), part)
    noise_key, walk_key, mix_key = jax.random.split(part_key, 3)
    weight_keys = jax.random.split(jax.random.key(seed + 1), 7)
    inner_width = HEADS * HEAD
    walk_path = jnp.cumsum(jax.random.normal(walk_key, (SEQ_LEN, WALK_RANK), jnp.float32), axis=0)
    walk_path = walk_path - jnp.mean(walk_path, axis=0, keepdims=True)
    walk_path = walk_path / jnp.sqrt(jnp.mean(walk_path * walk_path) + 1e-6)
    mixing = jax.random.normal(mix_key, (WALK_RANK, D), jnp.float32) * WALK_RANK ** -0.5
    x_val = 0.5 * jax.random.normal(noise_key, (SEQ_LEN, D), jnp.float32) + jnp.dot(walk_path, mixing)
    return {
        'x_in': x_val.astype(jnp.bfloat16),
        'g_attn': jax.random.uniform(weight_keys[0], (D,), jnp.float32, 0.5, 1.5),
        'w_qkv': (jax.random.normal(weight_keys[1], (D, 3 * inner_width), jnp.float32) * D ** -0.5).astype(jnp.bfloat16),
        'w_out': (jax.random.normal(weight_keys[2], (HEADS, HEAD, D), jnp.float32) * 1.5 * inner_width ** -0.5).astype(jnp.bfloat16),
        'g_mlp': jax.random.uniform(weight_keys[3], (D,), jnp.float32, 0.5, 1.5),
        'w_gate': (jax.random.normal(weight_keys[4], (D, FF), jnp.float32) * D ** -0.5).astype(jnp.bfloat16),
        'w_up': (jax.random.normal(weight_keys[5], (D, FF), jnp.float32) * D ** -0.5).astype(jnp.bfloat16),
        'w_down': (jax.random.normal(weight_keys[6], (FF, D), jnp.float32) * FF ** -0.5).astype(jnp.bfloat16),
    }


def rms_norm(row_vals, gain_vec):
    rows_f32 = row_vals.astype(jnp.float32)
    inv_rms = lax.rsqrt(jnp.mean(rows_f32 * rows_f32, axis=-1, keepdims=True) + 1e-5)
    return (rows_f32 * inv_rms * gain_vec).astype(jnp.bfloat16)


def rope_tables(positions):
    inv_freq = 1.0 / (ROPE_BASE ** (jnp.arange(0, HEAD, 2, dtype=jnp.float32) / HEAD))
    angles = positions.astype(jnp.float32)[:, None] * inv_freq[None, :]
    angles = jnp.concatenate([angles, angles], axis=-1)
    return jnp.cos(angles), jnp.sin(angles)


def apply_rope(qk_pair, cos_tab, sin_tab):
    half_dim = qk_pair.shape[-1] // 2
    rotated = jnp.concatenate([-qk_pair[..., half_dim:], qk_pair[..., :half_dim]], axis=-1)
    return qk_pair * cos_tab + rotated * sin_tab


def reference(x_in, g_attn, w_qkv, w_out, g_mlp, w_gate, w_up, w_down):
    inner_width = HEADS * HEAD
    x_norm = rms_norm(x_in, g_attn)
    qkv_f32 = jnp.dot(x_norm, w_qkv, preferred_element_type=jnp.float32).reshape(SEQ_LEN, 3, HEADS, HEAD)
    cos_tab, sin_tab = rope_tables(jnp.arange(SEQ_LEN))
    qk_rot = apply_rope(qkv_f32[:, :2], cos_tab[:, None, None, :], sin_tab[:, None, None, :])
    query_f32 = qk_rot[:, 0].astype(jnp.bfloat16).astype(jnp.float32)
    key_f32 = qk_rot[:, 1].astype(jnp.bfloat16).astype(jnp.float32)
    value_f32 = qkv_f32[:, 2].astype(jnp.bfloat16).astype(jnp.float32)
    score_scale = HEAD ** -0.5
    key_pos = jnp.arange(SEQ_LEN)

    def one_block(block_idx):
        row_start = block_idx * BLOCK_ROWS
        q_blk = lax.dynamic_slice_in_dim(query_f32, row_start, BLOCK_ROWS, axis=0)
        scores = jnp.einsum('qhd,khd->hqk', q_blk, key_f32) * score_scale
        query_pos = row_start + jnp.arange(BLOCK_ROWS)
        allowed = key_pos[None, :] <= query_pos[:, None]
        scores = jnp.where(allowed[None], scores, -jnp.inf)
        attn_probs = jax.nn.softmax(scores, axis=-1).astype(jnp.bfloat16).astype(jnp.float32)
        return jnp.einsum('hqk,khd->qhd', attn_probs, value_f32).astype(jnp.bfloat16)

    attn_rows = lax.map(one_block, jnp.arange(SEQ_LEN // BLOCK_ROWS)).reshape(SEQ_LEN, inner_width)
    attn_mixed = jnp.dot(attn_rows, w_out.reshape(inner_width, D), preferred_element_type=jnp.float32)
    y_rows = (x_in.astype(jnp.float32) + attn_mixed).astype(jnp.bfloat16)
    y_norm = rms_norm(y_rows, g_mlp)
    gate_pre = jnp.dot(y_norm, w_gate, preferred_element_type=jnp.float32)
    up_pre = jnp.dot(y_norm, w_up, preferred_element_type=jnp.float32)
    hidden = (jax.nn.silu(gate_pre) * up_pre).astype(jnp.bfloat16)
    return (y_rows.astype(jnp.float32) + jnp.dot(hidden, w_down, preferred_element_type=jnp.float32)).astype(jnp.bfloat16)
```

```python
import functools

import jax
import jax.numpy as jnp
from jax import lax
from jax.experimental import pallas as pl
from jax.experimental.pallas import tpu as pltpu
from jax.sharding import PartitionSpec as P

ROPE_BASE = 10000
F32 = jnp.float32
BF16 = jnp.bfloat16
LOG2E = 1.4426950408889634
VMEM_BYTES = 67_000_000
NEG = -1e30

PIECE = 128
QT = 256


def rope_tables(positions, head_dim):
    inv_freq = 1.0 / (ROPE_BASE ** (jnp.arange(0, head_dim, 2, dtype=F32) / head_dim))
    angles = positions.astype(F32)[:, None] * inv_freq[None, :]
    return jnp.cos(angles), jnp.sin(angles)


def _block_of(me, slot):
    chip = lax.rem(me // 2 + slot // 2, 2)
    core = lax.rem(lax.rem(me, 2) + lax.rem(slot, 2), 2)
    return chip * 2 + core


def attention_kernel(rows, heads, head_dim, x_hbm, g_ref, w_hbm, cos_ref, sin_ref, o_hbm,
                     xb, w, q_buf, k_buf, v_buf, xn, m_ref, l_ref, acc,
                     x_sem, w_sem, psend, precv, csend, crecv, dsend, drecv, osend, orecv, olocal):
    me = lax.axis_index('seq')
    hl = heads // 4
    n_chunks = rows // PIECE
    inner = heads * head_dim

    def w_copy(t, h):
        col = pl.multiple_of(t * inner + (me * hl + h) * head_dim, head_dim)
        return pltpu.make_async_copy(w_hbm.at[:, pl.ds(col, head_dim)], w.at[t * hl + h], w_sem.at[t * hl + h])

    x_local = pltpu.make_async_copy(x_hbm, xb.at[0], x_sem)
    x_local.start()
    for h in range(hl):
        for t in range(3):
            w_copy(t, h).start()

    barrier = pltpu.get_barrier_semaphore()
    for slot in (1, 2, 3):
        pl.semaphore_signal(barrier, inc=1, device_id={'seq': _block_of(me, slot)}, device_id_type=pl.DeviceIdType.MESH)
    pl.semaphore_wait(barrier, 3)

    def cross_copy(c):
        rs = pl.ds(c * PIECE, PIECE)
        return pltpu.make_async_remote_copy(
            src_ref=x_hbm.at[rs], dst_ref=xb.at[2, rs], send_sem=csend.at[c], recv_sem=crecv.at[c],
            device_id={'seq': _block_of(me, 2)}, device_id_type=pl.DeviceIdType.MESH)

    def diag_copy(c):
        rs = pl.ds(c * PIECE, PIECE)
        return pltpu.make_async_remote_copy(
            src_ref=xb.at[2, rs], dst_ref=xb.at[3, rs], send_sem=dsend.at[c], recv_sem=drecv.at[c],
            device_id={'seq': _block_of(me, 1)}, device_id_type=pl.DeviceIdType.MESH)

    partner = pltpu.make_async_remote_copy(
        src_ref=x_hbm, dst_ref=xb.at[1], send_sem=psend, recv_sem=precv,
        device_id={'seq': _block_of(me, 1)}, device_id_type=pl.DeviceIdType.MESH)
    for c in range(n_chunks):
        cross_copy(c).start()
    partner.start()
    x_local.wait()

    def project(j, slot, row, first):
        xf = xb[slot, pl.ds(row, PIECE), :].astype(F32)
        inv = lax.rsqrt(jnp.mean(xf * xf, axis=-1, keepdims=True) + 1e-5)
        xn[...] = (xf * inv * g_ref[...]).astype(BF16)
        base = pl.multiple_of(_block_of(me, slot) * rows + row, PIECE)
        cos_t = cos_ref[pl.ds(base, PIECE), :]
        sin_t = sin_ref[pl.ds(base, PIECE), :]
        half = head_dim // 2

        def one_head(h, _):
            for t, dst in ((0, q_buf), (1, k_buf), (2, v_buf)):
                @pl.when(j == 0)
                def _():
                    w_copy(t, h).wait()
                u = jnp.dot(xn[...], w[t * hl + h], preferred_element_type=F32)
                if t < 2:
                    a, b = u[:, :half], u[:, half:]
                    dst[h, pl.ds(base, PIECE), :half] = (a * cos_t - b * sin_t).astype(BF16)
                    dst[h, pl.ds(base, PIECE), half:] = (b * cos_t + a * sin_t).astype(BF16)
                else:
                    dst[h, pl.ds(base, PIECE), :] = u.astype(BF16)
            return 0
        lax.fori_loop(0, hl, one_head, 0)

    def piece(j, _):
        c = lax.rem(j, n_chunks)
        late = j // (2 * n_chunks)
        jj = j - 2 * n_chunks
        slot = (1 - late) * (j // n_chunks) + late * (2 + lax.rem(jj, 2))
        chunk = (1 - late) * c + late * (jj // 2)
        row = pl.multiple_of(chunk * PIECE, PIECE)

        @pl.when(j == n_chunks)
        def _():
            partner.wait_recv()

        @pl.when(slot == 2)
        def _():
            cross_copy(chunk).wait_recv()
            diag_copy(chunk).start()

        @pl.when(slot == 3)
        def _():
            diag_copy(chunk).wait_recv()

        project(j, slot, row, False)
        return 0

    lax.fori_loop(0, 4 * n_chunks, piece, 0)

    tiles = rows // QT
    scale = (head_dim ** -0.5) * LOG2E

    def unit(u):
        i = u // (2 * tiles)
        slot = (i + 2) * (1 - i // 2) + (3 - i) * (i // 2)
        tile = lax.rem(u // 2, tiles)
        hp = lax.rem(u, 2)
        return slot, tile, hp

    def out_remote(slot, tile, h):
        dst_block = _block_of(me, slot)
        src_row = pl.multiple_of(dst_block * rows + tile * QT, QT)
        col = pl.multiple_of((me * hl + h) * head_dim, head_dim)
        return pltpu.make_async_remote_copy(
            src_ref=q_buf.at[h, pl.ds(src_row, QT), :],
            dst_ref=o_hbm.at[pl.ds(pl.multiple_of(tile * QT, QT), QT), pl.ds(col, head_dim)],
            send_sem=osend.at[slot, tile, h], recv_sem=orecv.at[slot, tile, h],
            device_id={'seq': dst_block}, device_id_type=pl.DeviceIdType.MESH)

    def out_local(tile, h):
        src_row = pl.multiple_of(me * rows + tile * QT, QT)
        col = pl.multiple_of((me * hl + h) * head_dim, head_dim)
        return pltpu.make_async_copy(
            q_buf.at[h, pl.ds(src_row, QT), :],
            o_hbm.at[pl.ds(pl.multiple_of(tile * QT, QT), QT), pl.ds(col, head_dim)],
            olocal.at[tile, h])

    def send_unit(u):
        slot, tile, hp = unit(u)
        for d in range(2):
            h = hp * 2 + d

            @pl.when(slot > 0)
            def _():
                out_remote(slot, tile, h).start()

            @pl.when(slot == 0)
            def _():
                out_local(tile, h).start()

    def attend(u, _):
        slot, tile, hp = unit(u)
        block = _block_of(me, slot)
        qrow = pl.multiple_of(block * rows + tile * QT, QT)

        def scores(d, kc):
            h = hp * 2 + d
            kk = k_buf[h, pl.ds(pl.multiple_of(kc * rows, rows), rows), :]
            return lax.dot_general(q_buf[h, pl.ds(qrow, QT), :], kk, (((1,), (1,)), ((), ())), preferred_element_type=F32)

        def lane_sum(p):
            s = p[:, :128]
            for i in range(1, rows // 128):
                s = s + p[:, i * 128:(i + 1) * 128]
            return s

        for d in range(2):
            h = hp * 2 + d
            s = scores(d, block)
            ri = lax.broadcasted_iota(jnp.int32, (QT, rows), 0) + tile * QT
            ci = lax.broadcasted_iota(jnp.int32, (QT, rows), 1)
            s = jnp.where(ci <= ri, s, NEG)
            m = jnp.max(s, axis=-1, keepdims=True)
            p = jnp.exp2((s - m) * scale)
            m_ref[d] = jnp.broadcast_to(m, (QT, 128))
            l_ref[d] = lane_sum(p)
            vv = v_buf[h, pl.ds(pl.multiple_of(block * rows, rows), rows), :]
            acc[d] = jnp.dot(p.astype(BF16), vv, preferred_element_type=F32)

        def earlier(kc, _):
            for d in range(2):
                h = hp * 2 + d
                s = scores(d, kc)
                m_old = m_ref[d][:, :1]
                m = jnp.maximum(m_old, jnp.max(s, axis=-1, keepdims=True))
                alpha = jnp.exp2((m_old - m) * scale)
                p = jnp.exp2((s - m) * scale)
                m_ref[d] = jnp.broadcast_to(m, (QT, 128))
                l_ref[d] = l_ref[d] * alpha + lane_sum(p)
                vv = v_buf[h, pl.ds(pl.multiple_of(kc * rows, rows), rows), :]
                acc[d] = acc[d] * alpha + jnp.dot(p.astype(BF16), vv, preferred_element_type=F32)
            return 0
        lax.fori_loop(0, block, earlier, 0)

        for d in range(2):
            h = hp * 2 + d
            denom = jnp.sum(l_ref[d], axis=-1, keepdims=True)
            q_buf[h, pl.ds(qrow, QT), :] = (acc[d] / denom).astype(BF16)

        @pl.when(u > 0)
        def _():
            send_unit(u - 1)
        return 0

    n_units = 4 * tiles * 2
    lax.fori_loop(0, n_units, attend, 0)
    send_unit(n_units - 1)

    partner.wait_send()
    for c in range(n_chunks):
        cross_copy(c).wait_send()
        diag_copy(c).wait_send()
    for tile in range(tiles):
        for h in range(hl):
            out_local(tile, h).wait()
            for slot in (1, 2, 3):
                out_remote(slot, tile, h).wait_send()
                out_remote(slot, tile, h).wait_recv()


def attention(x_blk, g_attn, w_qkv, heads, head_dim):
    rows, width = x_blk.shape
    seq = 4 * rows
    hl = heads // 4
    n_chunks = rows // PIECE
    tiles = rows // QT
    cos_tab, sin_tab = rope_tables(jnp.arange(seq), head_dim)
    dma = pltpu.SemaphoreType.DMA
    anys = pl.BlockSpec(memory_space=pl.ANY)
    vm = pl.BlockSpec(memory_space=pltpu.VMEM)
    return pl.pallas_call(
        functools.partial(attention_kernel, rows, heads, head_dim),
        out_shape=jax.ShapeDtypeStruct((rows, heads * head_dim), BF16),
        in_specs=[anys, vm, anys, vm, vm],
        out_specs=anys,
        scratch_shapes=[
            pltpu.VMEM((4, rows, width), BF16),
            pltpu.VMEM((3 * hl, width, head_dim), BF16),
            pltpu.VMEM((hl, seq, head_dim), BF16),
            pltpu.VMEM((hl, seq, head_dim), BF16),
            pltpu.VMEM((hl, seq, head_dim), BF16),
            pltpu.VMEM((PIECE, width), BF16),
            pltpu.VMEM((2, QT, 128), F32),
            pltpu.VMEM((2, QT, 128), F32),
            pltpu.VMEM((2, QT, head_dim), F32),
            dma, dma((3 * hl,)), dma, dma,
            dma((n_chunks,)), dma((n_chunks,)), dma((n_chunks,)), dma((n_chunks,)),
            dma((4, tiles, hl)), dma((4, tiles, hl)), dma((tiles, hl)),
        ],
        compiler_params=pltpu.CompilerParams(
            collective_id=0, has_side_effects=True, vmem_limit_bytes=VMEM_BYTES),
        name='gather_attention',
    )(x_blk, g_attn.reshape(1, width), w_qkv, cos_tab, sin_tab)


def mlp_kernel(n_out, n_ff, bn, o_ref, x_ref, wo_ref, gm_ref, wg_ref, wu_ref, wd_ref, z_ref, acc, yn):
    i = pl.program_id(0)

    for s in range(n_out):
        @pl.when(i == s)
        def _():
            mixed = jnp.dot(o_ref[...], wo_ref[...], preferred_element_type=F32)
            y = (x_ref[...].astype(F32) + mixed).astype(BF16)
            acc[:, s * bn:(s + 1) * bn] = y.astype(F32)

    @pl.when(i == n_out)
    def _():
        y = acc[...]
        inv = lax.rsqrt(jnp.mean(y * y, axis=-1, keepdims=True) + 1e-5)
        yn[...] = (y * inv * gm_ref[...]).astype(BF16)

    @pl.when(i >= n_out)
    def _():
        gate = jnp.dot(yn[...], wg_ref[...], preferred_element_type=F32)
        up = jnp.dot(yn[...], wu_ref[...], preferred_element_type=F32)
        hidden = (gate * jax.nn.sigmoid(gate) * up).astype(BF16)
        width = acc.shape[1]
        step = width // 4
        for j in range(4):
            cs = slice(j * step, (j + 1) * step)
            acc[:, cs] += jnp.dot(hidden, wd_ref[:, cs], preferred_element_type=F32)

    @pl.when(i == n_out + n_ff - 1)
    def _():
        z_ref[...] = acc[...].astype(BF16)


def out_and_mlp(attn_rows, x_blk, w_out, g_mlp, w_gate, w_up, w_down):
    rows, width = x_blk.shape
    inner = attn_rows.shape[1]
    ff = w_gate.shape[1]
    bn = 512
    bf = 512
    n_out = width // bn
    n_ff = ff // bf
    one = pl.Buffered(1)
    c0 = lambda i: (0, 0)
    ffi = lambda i: jnp.maximum(i - n_out, 0)
    return pl.pallas_call(
        functools.partial(mlp_kernel, n_out, n_ff, bn),
        grid=(n_out + n_ff,),
        in_specs=[
            pl.BlockSpec((rows, inner), c0, pipeline_mode=one),
            pl.BlockSpec((rows, bn), lambda i: (0, jnp.minimum(i, n_out - 1))),
            pl.BlockSpec((inner, bn), lambda i: (0, jnp.minimum(i, n_out - 1))),
            pl.BlockSpec((1, width), c0, pipeline_mode=one),
            pl.BlockSpec((width, bf), lambda i: (0, ffi(i))),
            pl.BlockSpec((width, bf), lambda i: (0, ffi(i))),
            pl.BlockSpec((bf, width), lambda i: (ffi(i), 0)),
        ],
        out_specs=pl.BlockSpec((rows, width), c0, pipeline_mode=one),
        out_shape=jax.ShapeDtypeStruct((rows, width), BF16),
        scratch_shapes=[pltpu.VMEM((rows, width), F32), pltpu.VMEM((rows, width), BF16)],
        compiler_params=pltpu.CompilerParams(
            dimension_semantics=('arbitrary',), vmem_limit_bytes=VMEM_BYTES),
        name='out_mlp',
    )(attn_rows, x_blk, w_out, g_mlp.reshape(1, width), w_gate, w_up, w_down)


def solution(mesh):
    def local_layer(x_blk, g_attn, w_qkv, w_out, g_mlp, w_gate, w_up, w_down):
        n_heads, head_dim, model_width = w_out.shape
        attn_rows = attention(x_blk, g_attn, w_qkv, n_heads, head_dim)
        return out_and_mlp(attn_rows, x_blk, w_out.reshape(n_heads * head_dim, model_width), g_mlp, w_gate, w_up, w_down)

    row_spec = P(('data', 'seq'), None)
    return jax.shard_map(local_layer, mesh=mesh, in_specs=(row_spec, P(), P(), P(), P(), P(), P(), P()), out_specs=row_spec, check_vma=False)
```

```python
import functools

import jax
import jax.numpy as jnp
from jax import lax
from jax.experimental import pallas as pl
from jax.experimental.pallas import tpu as pltpu
from jax.sharding import PartitionSpec as P

ROPE_BASE = 10000
F32 = jnp.float32
BF16 = jnp.bfloat16
LOG2E = 1.4426950408889634
VMEM_BYTES = 67_000_000
NEG = -1e30

PIECE = 128
CHUNK = 64
QT = 256


def rope_tables(seq, head_dim):
    inv_freq = 1.0 / (ROPE_BASE ** (jnp.arange(0, head_dim, 2, dtype=F32) / head_dim))
    positions = jnp.concatenate([jnp.arange(PIECE), jnp.arange(0, seq, PIECE)])
    angles = positions.astype(F32)[:, None] * inv_freq[None, :]
    return jnp.cos(angles), jnp.sin(angles)


def _block_of(me, slot):
    chip = lax.rem(me // 2 + slot // 2, 2)
    core = lax.rem(lax.rem(me, 2) + lax.rem(slot, 2), 2)
    return chip * 2 + core


def attention_kernel(rows, heads, head_dim, x_hbm, g_ref, w_hbm, cos_ref, sin_ref, o_hbm,
                     xb, w, q_buf, k_buf, v_buf, xn, tab, m_ref, l_ref, acc,
                     x_sem, w_sem, psend, precv, csend, crecv, dsend, drecv, osend, orecv, olocal):
    me = lax.axis_index('seq')
    hl = heads // 4
    n_pieces = rows // PIECE
    n_chunks = rows // CHUNK
    core = lax.rem(me, 2)
    inner = heads * head_dim

    def w_copy(t, h):
        col = pl.multiple_of(t * inner + (me * hl + h) * head_dim, head_dim)
        return pltpu.make_async_copy(w_hbm.at[:, pl.ds(col, head_dim)], w.at[t * hl + h], w_sem.at[t * hl + h])

    x_local = pltpu.make_async_copy(x_hbm, xb.at[0], x_sem)
    x_local.start()
    for t in range(3):
        w_copy(t, 0).start()

    barrier = pltpu.get_barrier_semaphore()
    for slot in (1, 2, 3):
        pl.semaphore_signal(barrier, inc=1, device_id={'seq': _block_of(me, slot)}, device_id_type=pl.DeviceIdType.MESH)
    pl.semaphore_wait(barrier, 3)

    def cross_copy(c):
        rs = pl.ds(pl.multiple_of(c * CHUNK, CHUNK), CHUNK)
        return pltpu.make_async_remote_copy(
            src_ref=x_hbm.at[rs], dst_ref=xb.at[2, rs], send_sem=csend.at[c], recv_sem=crecv.at[c],
            device_id={'seq': _block_of(me, 2)}, device_id_type=pl.DeviceIdType.MESH)

    def diag_copy(c):
        rs = pl.ds(pl.multiple_of(c * CHUNK, CHUNK), CHUNK)
        return pltpu.make_async_remote_copy(
            src_ref=xb.at[2, rs], dst_ref=xb.at[3, rs], send_sem=dsend.at[c], recv_sem=drecv.at[c],
            device_id={'seq': _block_of(me, 1)}, device_id_type=pl.DeviceIdType.MESH)

    partner = pltpu.make_async_remote_copy(
        src_ref=x_hbm, dst_ref=xb.at[1], send_sem=psend, recv_sem=precv,
        device_id={'seq': _block_of(me, 1)}, device_id_type=pl.DeviceIdType.MESH)
    cross_copy(0).start()
    partner.start()
    x_local.wait()
    for h in range(1, hl):
        for t in range(3):
            w_copy(t, h).start()

    def norm_rows(slot, row, count, at):
        width = g_ref.shape[1]
        cw = 1024
        for r in range(0, count, 16):
            rs = pl.ds(pl.multiple_of(row + r, 16), 16)
            total = jnp.zeros((16, 128), F32)
            for c in range(0, width, cw):
                xf = xb[slot, rs, c:c + cw].astype(F32)
                sq = xf * xf
                for i in range(0, cw, 128):
                    total = total + sq[:, i:i + 128]
            inv = lax.rsqrt(jnp.sum(total, axis=-1, keepdims=True) / width + 1e-5)
            for c in range(0, width, cw):
                xf = xb[slot, rs, c:c + cw].astype(F32)
                xn[at + r:at + r + 16, c:c + cw] = (xf * inv * g_ref[:, c:c + cw]).astype(BF16)

    half = head_dim // 2

    def project(first, bases):
        run = PIECE // len(bases)
        tabs = []
        for i, base in enumerate(bases):
            low = lax.rem(base, PIECE)
            c0 = cos_ref[pl.ds(pl.multiple_of(low, run), run), :]
            s0 = sin_ref[pl.ds(pl.multiple_of(low, run), run), :]
            c1 = cos_ref[pl.ds(PIECE + base // PIECE, 1), :]
            s1 = sin_ref[pl.ds(PIECE + base // PIECE, 1), :]
            tabs.append((c0 * c1 - s0 * s1, s0 * c1 + c0 * s1))
        cos_t = jnp.concatenate([t[0] for t in tabs], axis=0)
        sin_t = jnp.concatenate([t[1] for t in tabs], axis=0)
        tab[0] = cos_t
        tab[1] = sin_t

        def one_head(h, _):
            if first is not None:
                @pl.when(first)
                def _():
                    for t in range(3):
                        w_copy(t, h).wait()
            for t, dst in ((0, q_buf), (1, k_buf), (2, v_buf)):
                u = jnp.dot(xn[...], w[t * hl + h], preferred_element_type=F32)
                if t < 2:
                    a, b = u[:, :half], u[:, half:]
                    parts = ((0, (a * tab[0] - b * tab[1]).astype(BF16)), (half, (b * tab[0] + a * tab[1]).astype(BF16)))
                else:
                    parts = ((0, u.astype(BF16)),)
                for off, val in parts:
                    for i, base in enumerate(bases):
                        dst[h, pl.ds(pl.multiple_of(base, run), run), off:off + val.shape[1]] = val[i * run:(i + 1) * run]
            return 0
        lax.fori_loop(0, hl, one_head, 0)

    def near_piece(j, _):
        slot = j // n_pieces
        row = pl.multiple_of(lax.rem(j, n_pieces) * PIECE, PIECE)

        @pl.when(j == n_pieces)
        def _():
            partner.wait_recv()

        norm_rows(slot, row, PIECE, 0)
        project(j == 0, [_block_of(me, slot) * rows + row])

        @pl.when(j == 0)
        def _():
            cross_copy(1).start()

        @pl.when((j >= 3) & (lax.rem(j, 2) == 1))
        def _():
            done = (j - 3) // 2
            cross_copy(done).wait_send()
            cross_copy(done + 2).start()
        return 0

    lax.fori_loop(0, 2 * n_pieces, near_piece, 0)
    n_near = n_pieces - 1

    tiles = rows // QT
    scale = (head_dim ** -0.5) * LOG2E

    def unit(u):
        i = u // (2 * tiles)
        far = 2 + lax.rem(i + core, 2)
        slot = far * (1 - i // 2) + (3 - i) * (i // 2)
        tile = lax.rem(u // 2, tiles)
        hp = lax.rem(u, 2)
        return slot, tile, hp

    def out_remote(slot, tile, h):
        dst_block = _block_of(me, slot)
        src_row = pl.multiple_of(dst_block * rows + tile * QT, QT)
        col = pl.multiple_of((me * hl + h) * head_dim, head_dim)
        return pltpu.make_async_remote_copy(
            src_ref=q_buf.at[h, pl.ds(src_row, QT), :],
            dst_ref=o_hbm.at[pl.ds(pl.multiple_of(tile * QT, QT), QT), pl.ds(col, head_dim)],
            send_sem=osend.at[slot, tile, h], recv_sem=orecv.at[slot, tile, h],
            device_id={'seq': dst_block}, device_id_type=pl.DeviceIdType.MESH)

    def out_local(tile, h):
        src_row = pl.multiple_of(me * rows + tile * QT, QT)
        col = pl.multiple_of((me * hl + h) * head_dim, head_dim)
        return pltpu.make_async_copy(
            q_buf.at[h, pl.ds(src_row, QT), :],
            o_hbm.at[pl.ds(pl.multiple_of(tile * QT, QT), QT), pl.ds(col, head_dim)],
            olocal.at[tile, h])

    def send_unit(u):
        slot, tile, hp = unit(u)
        for d in range(2):
            h = hp * 2 + d

            @pl.when(slot > 0)
            def _():
                out_remote(slot, tile, h).start()

            @pl.when(slot == 0)
            def _():
                out_local(tile, h).start()

    def attend(u):
        slot, tile, hp = unit(u)
        block = _block_of(me, slot)
        first = pl.multiple_of(block * rows, rows)
        qrow = pl.multiple_of(first + tile * QT, QT)

        def scores(d, row, count):
            h = hp * 2 + d
            kk = k_buf[h, pl.ds(row, count), :]
            return lax.dot_general(q_buf[h, pl.ds(qrow, QT), :], kk, (((1,), (1,)), ((), ())), preferred_element_type=F32)

        def lane_sum(p):
            s = p[:, :128]
            for i in range(128, p.shape[1], 128):
                s = s + p[:, i:i + 128]
            return s

        for d in range(2):
            h = hp * 2 + d
            s = scores(d, qrow, QT)
            ri = lax.broadcasted_iota(jnp.int32, (QT, QT), 0)
            ci = lax.broadcasted_iota(jnp.int32, (QT, QT), 1)
            s = jnp.where(ci <= ri, s, NEG)
            m = jnp.max(s, axis=-1, keepdims=True)
            p = jnp.exp2((s - m) * scale)
            m_ref[d] = jnp.broadcast_to(m, (QT, 128))
            l_ref[d] = lane_sum(p)
            acc[d] = jnp.dot(p.astype(BF16), v_buf[h, pl.ds(qrow, QT), :], preferred_element_type=F32)

        def update(row, count):
            for d in range(2):
                h = hp * 2 + d
                s = scores(d, row, count)
                m_old = m_ref[d][:, :1]
                m = jnp.maximum(m_old, jnp.max(s, axis=-1, keepdims=True))
                alpha = jnp.exp2((m_old - m) * scale)
                p = jnp.exp2((s - m) * scale)
                m_ref[d] = jnp.broadcast_to(m, (QT, 128))
                l_ref[d] = l_ref[d] * alpha + lane_sum(p)
                acc[d] = acc[d] * alpha + jnp.dot(p.astype(BF16), v_buf[h, pl.ds(row, count), :], preferred_element_type=F32)

        def earlier_tile(kt, _):
            update(pl.multiple_of(first + kt * QT, QT), QT)
            return 0
        lax.fori_loop(0, tile, earlier_tile, 0)

        def earlier_block(kb, _):
            update(pl.multiple_of(kb * rows, rows), rows)
            return 0
        lax.fori_loop(0, block, earlier_block, 0)

        for d in range(2):
            h = hp * 2 + d
            denom = jnp.sum(l_ref[d], axis=-1, keepdims=True)
            q_buf[h, pl.ds(qrow, QT), :] = (acc[d] / denom).astype(BF16)

    early = rows // CHUNK // tiles
    n_early = 2
    n_units = 4 * tiles * 2

    def far_step(i, _):
        is_unit = ((i >= early) & (i < early + n_early)) | (i >= n_chunks + n_early)

        @pl.when(jnp.logical_not(is_unit))
        def _():
            k = i - n_early * ((i >= early).astype(jnp.int32))
            cross_copy(k).wait_recv()
            diag_copy(k).start()

            @pl.when((k >= n_near) & (k < n_chunks - 2))
            def _():
                cross_copy(k).wait_send()
                cross_copy(k + 2).start()

            @pl.when(k == n_chunks - 1)
            def _():
                for u in range(n_early):
                    send_unit(u)
            row = pl.multiple_of(k * CHUNK, CHUNK)
            norm_rows(2, row, CHUNK, 0)
            diag_copy(k).wait_recv()
            norm_rows(3, row, CHUNK, CHUNK)
            project(None, [_block_of(me, 2) * rows + row, _block_of(me, 3) * rows + row])

        @pl.when(is_unit)
        def _():
            u = i - early * (1 - (i >= n_chunks + n_early).astype(jnp.int32)) - n_chunks * ((i >= n_chunks + n_early).astype(jnp.int32))
            attend(u)

            @pl.when(u > n_early)
            def _():
                send_unit(u - 1)
        return 0

    lax.fori_loop(0, n_chunks + n_units, far_step, 0)
    send_unit(n_units - 1)

    partner.wait_send()
    for c in range(n_chunks):
        if c >= n_chunks - 2:
            cross_copy(c).wait_send()
        diag_copy(c).wait_send()
    for tile in range(tiles):
        for h in range(hl):
            out_local(tile, h).wait()
            for slot in (1, 2, 3):
                out_remote(slot, tile, h).wait_send()
                out_remote(slot, tile, h).wait_recv()


def attention(x_blk, g_attn, w_qkv, heads, head_dim):
    rows, width = x_blk.shape
    seq = 4 * rows
    hl = heads // 4
    n_chunks = rows // CHUNK
    tiles = rows // QT
    cos_tab, sin_tab = rope_tables(seq, head_dim)
    dma = pltpu.SemaphoreType.DMA
    anys = pl.BlockSpec(memory_space=pl.ANY)
    vm = pl.BlockSpec(memory_space=pltpu.VMEM)
    return pl.pallas_call(
        functools.partial(attention_kernel, rows, heads, head_dim),
        out_shape=jax.ShapeDtypeStruct((rows, heads * head_dim), BF16),
        in_specs=[anys, vm, anys, vm, vm],
        out_specs=anys,
        scratch_shapes=[
            pltpu.VMEM((4, rows, width), BF16),
            pltpu.VMEM((3 * hl, width, head_dim), BF16),
            pltpu.VMEM((hl, seq, head_dim), BF16),
            pltpu.VMEM((hl, seq, head_dim), BF16),
            pltpu.VMEM((hl, seq, head_dim), BF16),
            pltpu.VMEM((PIECE, width), BF16),
            pltpu.VMEM((2, PIECE, head_dim // 2), F32),
            pltpu.VMEM((2, QT, 128), F32),
            pltpu.VMEM((2, QT, 128), F32),
            pltpu.VMEM((2, QT, head_dim), F32),
            dma, dma((3 * hl,)), dma, dma,
            dma((n_chunks,)), dma((n_chunks,)), dma((n_chunks,)), dma((n_chunks,)),
            dma((4, tiles, hl)), dma((4, tiles, hl)), dma((tiles, hl)),
        ],
        compiler_params=pltpu.CompilerParams(
            collective_id=0, has_side_effects=True, vmem_limit_bytes=VMEM_BYTES),
        name='gather_attention',
    )(x_blk, g_attn.reshape(1, width), w_qkv, cos_tab, sin_tab)


def mlp_kernel(n_out, n_ff, bn, o_ref, x_ref, wo_ref, gm_ref, wg_ref, wu_ref, wd_ref, z_ref, acc, yn):
    i = pl.program_id(0)

    for s in range(n_out):
        @pl.when(i == s)
        def _():
            mixed = jnp.dot(o_ref[...], wo_ref[...], preferred_element_type=F32)
            y = (x_ref[...].astype(F32) + mixed).astype(BF16)
            acc[:, s * bn:(s + 1) * bn] = y.astype(F32)

    @pl.when(i == n_out)
    def _():
        n_rows, width = acc.shape
        cw = 1024

        def slab(r, _):
            rs = pl.ds(pl.multiple_of(r * 32, 32), 32)
            total = jnp.zeros((32, 128), F32)
            for c in range(0, width, cw):
                y = acc[rs, c:c + cw]
                sq = y * y
                for k in range(0, cw, 128):
                    total = total + sq[:, k:k + 128]
            inv = lax.rsqrt(jnp.sum(total, axis=-1, keepdims=True) / width + 1e-5)
            for c in range(0, width, cw):
                yn[rs, c:c + cw] = (acc[rs, c:c + cw] * inv * gm_ref[:, c:c + cw]).astype(BF16)
            return 0
        lax.fori_loop(0, n_rows // 32, slab, 0, unroll=2)

    @pl.when(i >= n_out)
    def _():
        gate = jnp.dot(yn[...], wg_ref[...], preferred_element_type=F32)
        up = jnp.dot(yn[...], wu_ref[...], preferred_element_type=F32)
        hidden = (gate * jax.nn.sigmoid(gate) * up).astype(BF16)
        width = acc.shape[1]
        step = width // 4
        for j in range(4):
            cs = slice(j * step, (j + 1) * step)
            acc[:, cs] += jnp.dot(hidden, wd_ref[:, cs], preferred_element_type=F32)

    @pl.when(i == n_out + n_ff - 1)
    def _():
        z_ref[...] = acc[...].astype(BF16)


def out_and_mlp(attn_rows, x_blk, w_out, g_mlp, w_gate, w_up, w_down):
    rows, width = x_blk.shape
    inner = attn_rows.shape[1]
    ff = w_gate.shape[1]
    bn = 512
    bf = 512
    n_out = width // bn
    n_ff = ff // bf
    one = pl.Buffered(1)
    c0 = lambda i: (0, 0)
    ffi = lambda i: jnp.maximum(i - n_out, 0)
    return pl.pallas_call(
        functools.partial(mlp_kernel, n_out, n_ff, bn),
        grid=(n_out + n_ff,),
        in_specs=[
            pl.BlockSpec((rows, inner), c0, pipeline_mode=one),
            pl.BlockSpec((rows, bn), lambda i: (0, jnp.minimum(i, n_out - 1))),
            pl.BlockSpec((inner, bn), lambda i: (0, jnp.minimum(i, n_out - 1))),
            pl.BlockSpec((1, width), c0, pipeline_mode=one),
            pl.BlockSpec((width, bf), lambda i: (0, ffi(i))),
            pl.BlockSpec((width, bf), lambda i: (0, ffi(i))),
            pl.BlockSpec((bf, width), lambda i: (ffi(i), 0)),
        ],
        out_specs=pl.BlockSpec((rows, width), c0, pipeline_mode=one),
        out_shape=jax.ShapeDtypeStruct((rows, width), BF16),
        scratch_shapes=[pltpu.VMEM((rows, width), F32), pltpu.VMEM((rows, width), BF16)],
        compiler_params=pltpu.CompilerParams(
            dimension_semantics=('arbitrary',), vmem_limit_bytes=VMEM_BYTES),
        name='out_mlp',
    )(attn_rows, x_blk, w_out, g_mlp.reshape(1, width), w_gate, w_up, w_down)


def solution(mesh):
    def local_layer(x_blk, g_attn, w_qkv, w_out, g_mlp, w_gate, w_up, w_down):
        n_heads, head_dim, model_width = w_out.shape
        attn_rows = attention(x_blk, g_attn, w_qkv, n_heads, head_dim)
        return out_and_mlp(attn_rows, x_blk, w_out.reshape(n_heads * head_dim, model_width), g_mlp, w_gate, w_up, w_down)

    row_spec = P(('data', 'seq'), None)
    return jax.shard_map(local_layer, mesh=mesh, in_specs=(row_spec, P(), P(), P(), P(), P(), P(), P()), out_specs=row_spec, check_vma=False)
```

```python
import functools

import jax
import jax.numpy as jnp
from jax import lax
from jax.experimental import pallas as pl
from jax.experimental.pallas import tpu as pltpu
from jax.sharding import PartitionSpec as P

ROPE_BASE = 10000
F32 = jnp.float32
BF16 = jnp.bfloat16
LOG2E = 1.4426950408889634
VMEM_BYTES = 67_000_000
NEG = -1e30

PIECE = 128
CHUNK = 64
QT = 256


def rope_tables(seq, head_dim):
    inv_freq = 1.0 / (ROPE_BASE ** (jnp.arange(0, head_dim, 2, dtype=F32) / head_dim))
    positions = jnp.concatenate([jnp.arange(PIECE), jnp.arange(0, seq, PIECE)])
    angles = positions.astype(F32)[:, None] * inv_freq[None, :]
    return jnp.cos(angles), jnp.sin(angles)


def _block_of(me, slot):
    chip = lax.rem(me // 2 + slot // 2, 2)
    core = lax.rem(lax.rem(me, 2) + lax.rem(slot, 2), 2)
    return chip * 2 + core


def attention_kernel(rows, heads, head_dim, x_hbm, g_ref, w_hbm, cos_ref, sin_ref, o_hbm,
                     xb, w, q_buf, k_buf, v_buf, xn, tab, m_ref, l_ref, acc,
                     x_sem, w_sem, psend, precv, csend, crecv, dsend, drecv, osend, orecv, olocal):
    me = lax.axis_index('seq')
    hl = heads // 4
    n_pieces = rows // PIECE
    n_chunks = rows // CHUNK
    core = lax.rem(me, 2)
    inner = heads * head_dim

    def w_copy(t, h):
        col = pl.multiple_of(t * inner + (me * hl + h) * head_dim, head_dim)
        return pltpu.make_async_copy(w_hbm.at[:, pl.ds(col, head_dim)], w.at[t * hl + h], w_sem.at[t * hl + h])

    x_local = pltpu.make_async_copy(x_hbm, xb.at[0], x_sem)
    x_local.start()
    for t in range(3):
        w_copy(t, 0).start()

    barrier = pltpu.get_barrier_semaphore()
    for slot in (1, 2, 3):
        pl.semaphore_signal(barrier, inc=1, device_id={'seq': _block_of(me, slot)}, device_id_type=pl.DeviceIdType.MESH)
    pl.semaphore_wait(barrier, 3)

    def cross_copy(c):
        rs = pl.ds(pl.multiple_of(c * CHUNK, CHUNK), CHUNK)
        return pltpu.make_async_remote_copy(
            src_ref=x_hbm.at[rs], dst_ref=xb.at[2, rs], send_sem=csend.at[c], recv_sem=crecv.at[c],
            device_id={'seq': _block_of(me, 2)}, device_id_type=pl.DeviceIdType.MESH)

    def diag_copy(c):
        rs = pl.ds(pl.multiple_of(c * CHUNK, CHUNK), CHUNK)
        return pltpu.make_async_remote_copy(
            src_ref=xb.at[2, rs], dst_ref=xb.at[3, rs], send_sem=dsend.at[c], recv_sem=drecv.at[c],
            device_id={'seq': _block_of(me, 1)}, device_id_type=pl.DeviceIdType.MESH)

    partner = pltpu.make_async_remote_copy(
        src_ref=x_hbm, dst_ref=xb.at[1], send_sem=psend, recv_sem=precv,
        device_id={'seq': _block_of(me, 1)}, device_id_type=pl.DeviceIdType.MESH)
    cross_copy(0).start()
    partner.start()
    x_local.wait()
    for h in range(1, hl):
        for t in range(3):
            w_copy(t, h).start()

    def norm_rows(slot, row, count, at):
        width = g_ref.shape[1]
        cw = 1024
        for r in range(0, count, 16):
            rs = pl.ds(pl.multiple_of(row + r, 16), 16)
            total = jnp.zeros((16, 128), F32)
            for c in range(0, width, cw):
                xf = xb[slot, rs, c:c + cw].astype(F32)
                sq = xf * xf
                for i in range(0, cw, 128):
                    total = total + sq[:, i:i + 128]
            inv = lax.rsqrt(jnp.sum(total, axis=-1, keepdims=True) / width + 1e-5)
            for c in range(0, width, cw):
                xf = xb[slot, rs, c:c + cw].astype(F32)
                xn[at + r:at + r + 16, c:c + cw] = (xf * inv * g_ref[:, c:c + cw]).astype(BF16)

    half = head_dim // 2

    def project(first, bases):
        run = PIECE // len(bases)
        tabs = []
        for i, base in enumerate(bases):
            low = lax.rem(base, PIECE)
            c0 = cos_ref[pl.ds(pl.multiple_of(low, run), run), :]
            s0 = sin_ref[pl.ds(pl.multiple_of(low, run), run), :]
            c1 = cos_ref[pl.ds(PIECE + base // PIECE, 1), :]
            s1 = sin_ref[pl.ds(PIECE + base // PIECE, 1), :]
            tabs.append((c0 * c1 - s0 * s1, s0 * c1 + c0 * s1))
        cos_t = jnp.concatenate([t[0] for t in tabs], axis=0)
        sin_t = jnp.concatenate([t[1] for t in tabs], axis=0)
        tab[0] = cos_t
        tab[1] = sin_t

        def one_head(h, _):
            if first is not None:
                @pl.when(first)
                def _():
                    for t in range(3):
                        w_copy(t, h).wait()
            for t, dst in ((0, q_buf), (1, k_buf), (2, v_buf)):
                u = jnp.dot(xn[...], w[t * hl + h], preferred_element_type=F32)
                if t < 2:
                    a, b = u[:, :half], u[:, half:]
                    parts = ((0, (a * tab[0] - b * tab[1]).astype(BF16)), (half, (b * tab[0] + a * tab[1]).astype(BF16)))
                else:
                    parts = ((0, u.astype(BF16)),)
                for off, val in parts:
                    for i, base in enumerate(bases):
                        dst[h, pl.ds(pl.multiple_of(base, run), run), off:off + val.shape[1]] = val[i * run:(i + 1) * run]
            return 0
        lax.fori_loop(0, hl, one_head, 0)

    def near_piece(j, _):
        slot = j // n_pieces
        row = pl.multiple_of(lax.rem(j, n_pieces) * PIECE, PIECE)

        @pl.when(j == n_pieces)
        def _():
            partner.wait_recv()

        norm_rows(slot, row, PIECE, 0)
        project(j == 0, [_block_of(me, slot) * rows + row])

        @pl.when(j == 0)
        def _():
            cross_copy(1).start()

        @pl.when((j >= 3) & (lax.rem(j, 2) == 1))
        def _():
            done = (j - 3) // 2
            cross_copy(done).wait_send()
            cross_copy(done + 2).start()
        return 0

    lax.fori_loop(0, 2 * n_pieces, near_piece, 0)
    n_near = n_pieces - 1

    tiles = rows // QT
    scale = (head_dim ** -0.5) * LOG2E

    def unit(u):
        i = u // (2 * tiles)
        far = 2 + lax.rem(i + core, 2)
        slot = far * (1 - i // 2) + (3 - i) * (i // 2)
        tile = lax.rem(u // 2, tiles)
        hp = lax.rem(u, 2)
        return slot, tile, hp

    def out_remote(slot, tile, h):
        dst_block = _block_of(me, slot)
        src_row = pl.multiple_of(dst_block * rows + tile * QT, QT)
        col = pl.multiple_of((me * hl + h) * head_dim, head_dim)
        return pltpu.make_async_remote_copy(
            src_ref=q_buf.at[h, pl.ds(src_row, QT), :],
            dst_ref=o_hbm.at[pl.ds(pl.multiple_of(tile * QT, QT), QT), pl.ds(col, head_dim)],
            send_sem=osend.at[slot, tile, h], recv_sem=orecv.at[slot, tile, h],
            device_id={'seq': dst_block}, device_id_type=pl.DeviceIdType.MESH)

    def out_local(tile, h):
        src_row = pl.multiple_of(me * rows + tile * QT, QT)
        col = pl.multiple_of((me * hl + h) * head_dim, head_dim)
        return pltpu.make_async_copy(
            q_buf.at[h, pl.ds(src_row, QT), :],
            o_hbm.at[pl.ds(pl.multiple_of(tile * QT, QT), QT), pl.ds(col, head_dim)],
            olocal.at[tile, h])

    def send_unit(u):
        slot, tile, hp = unit(u)
        for d in range(2):
            h = hp * 2 + d

            @pl.when(slot > 0)
            def _():
                out_remote(slot, tile, h).start()

            @pl.when(slot == 0)
            def _():
                out_local(tile, h).start()

    def attend(u):
        slot, tile, hp = unit(u)
        block = _block_of(me, slot)
        first = pl.multiple_of(block * rows, rows)
        qrow = pl.multiple_of(first + tile * QT, QT)

        def scores(d, row, count):
            h = hp * 2 + d
            kk = k_buf[h, pl.ds(row, count), :]
            return lax.dot_general(kk, q_buf[h, pl.ds(qrow, QT), :], (((1,), (1,)), ((), ())), preferred_element_type=F32)

        def weigh(d, row, count, p):
            vv = v_buf[hp * 2 + d, pl.ds(row, count), :]
            return lax.dot_general(vv, p.astype(BF16), (((0,), (0,)), ((), ())), preferred_element_type=F32)

        s_all = [scores(d, qrow, QT) for d in range(2)]
        for d in range(2):
            ki = lax.broadcasted_iota(jnp.int32, (QT, QT), 0)
            qi = lax.broadcasted_iota(jnp.int32, (QT, QT), 1)
            s = jnp.where(ki <= qi, s_all[d], NEG)
            m = jnp.max(s, axis=0, keepdims=True)
            p = jnp.exp2((s - m) * scale)
            m_ref[d] = m
            l_ref[d] = jnp.sum(p, axis=0, keepdims=True)
            acc[d] = weigh(d, qrow, QT, p)

        def update(row, count):
            s_all = [scores(d, row, count) for d in range(2)]
            for d in range(2):
                s = s_all[d]
                m_old = m_ref[d]
                m = jnp.maximum(m_old, jnp.max(s, axis=0, keepdims=True))
                alpha = jnp.exp2((m_old - m) * scale)
                p = jnp.exp2((s - m) * scale)
                m_ref[d] = m
                l_ref[d] = l_ref[d] * alpha + jnp.sum(p, axis=0, keepdims=True)
                acc[d] = acc[d] * alpha + weigh(d, row, count, p)

        def earlier_tile(kt, _):
            update(pl.multiple_of(first + kt * QT, QT), QT)
            return 0
        lax.fori_loop(0, tile, earlier_tile, 0)

        def earlier_block(kb, _):
            update(pl.multiple_of(kb * rows, rows), rows)
            return 0
        lax.fori_loop(0, block, earlier_block, 0)

        for d in range(2):
            h = hp * 2 + d
            out = acc[d] * (1.0 / l_ref[d])
            q_buf[h, pl.ds(qrow, QT), :] = jnp.transpose(out).astype(BF16)

    early = rows // CHUNK // tiles
    n_early = 2
    n_units = 4 * tiles * 2
    assert n_chunks == 8 and n_near == 3

    def far_step(i, _):
        is_unit = ((i >= early) & (i < early + n_early)) | (i >= n_chunks + n_early)

        @pl.when(jnp.logical_not(is_unit))
        def _():
            k = i - n_early * ((i >= early).astype(jnp.int32))
            cross_copy(k).wait_recv()
            diag_copy(k).start()

            @pl.when((k == 2) | (k == 5))
            def _():
                done = n_near + 2 * ((k - 2) // 3)
                cross_copy(done).wait_send()
                cross_copy(done + 2).start()

            @pl.when(k == n_chunks - 1)
            def _():
                for u in range(n_early):
                    send_unit(u)
            row = pl.multiple_of(k * CHUNK, CHUNK)
            norm_rows(2, row, CHUNK, 0)
            diag_copy(k).wait_recv()
            norm_rows(3, row, CHUNK, CHUNK)
            project(None, [_block_of(me, 2) * rows + row, _block_of(me, 3) * rows + row])

        @pl.when(is_unit)
        def _():
            u = i - early * (1 - (i >= n_chunks + n_early).astype(jnp.int32)) - n_chunks * ((i >= n_chunks + n_early).astype(jnp.int32))
            attend(u)

            @pl.when(u == 0)
            def _():
                cross_copy(n_near + 1).wait_send()
                cross_copy(n_near + 3).start()

            @pl.when(u > n_early)
            def _():
                send_unit(u - 1)
        return 0

    lax.fori_loop(0, n_chunks + n_units, far_step, 0)
    send_unit(n_units - 1)

    partner.wait_send()
    for c in range(n_chunks):
        if c >= n_chunks - 2:
            cross_copy(c).wait_send()
        diag_copy(c).wait_send()
    for tile in range(tiles):
        for h in range(hl):
            out_local(tile, h).wait()
            for slot in (1, 2, 3):
                out_remote(slot, tile, h).wait_send()
                out_remote(slot, tile, h).wait_recv()


def attention(x_blk, g_attn, w_qkv, heads, head_dim):
    rows, width = x_blk.shape
    seq = 4 * rows
    hl = heads // 4
    n_chunks = rows // CHUNK
    tiles = rows // QT
    cos_tab, sin_tab = rope_tables(seq, head_dim)
    dma = pltpu.SemaphoreType.DMA
    anys = pl.BlockSpec(memory_space=pl.ANY)
    vm = pl.BlockSpec(memory_space=pltpu.VMEM)
    return pl.pallas_call(
        functools.partial(attention_kernel, rows, heads, head_dim),
        out_shape=jax.ShapeDtypeStruct((rows, heads * head_dim), BF16),
        in_specs=[anys, vm, anys, vm, vm],
        out_specs=anys,
        scratch_shapes=[
            pltpu.VMEM((4, rows, width), BF16),
            pltpu.VMEM((3 * hl, width, head_dim), BF16),
            pltpu.VMEM((hl, seq, head_dim), BF16),
            pltpu.VMEM((hl, seq, head_dim), BF16),
            pltpu.VMEM((hl, seq, head_dim), BF16),
            pltpu.VMEM((PIECE, width), BF16),
            pltpu.VMEM((2, PIECE, head_dim // 2), F32),
            pltpu.VMEM((2, 1, QT), F32),
            pltpu.VMEM((2, 1, QT), F32),
            pltpu.VMEM((2, head_dim, QT), F32),
            dma, dma((3 * hl,)), dma, dma,
            dma((n_chunks,)), dma((n_chunks,)), dma((n_chunks,)), dma((n_chunks,)),
            dma((4, tiles, hl)), dma((4, tiles, hl)), dma((tiles, hl)),
        ],
        compiler_params=pltpu.CompilerParams(
            collective_id=0, has_side_effects=True, vmem_limit_bytes=VMEM_BYTES),
        name='gather_attention',
    )(x_blk, g_attn.reshape(1, width), w_qkv, cos_tab, sin_tab)


def mlp_kernel(n_out, n_ff, bn, o_ref, x_ref, wo_ref, gm_ref, wg_ref, wu_ref, wd_ref, z_ref, acc, yn):
    i = pl.program_id(0)

    for s in range(n_out):
        @pl.when(i == s)
        def _():
            mixed = jnp.dot(o_ref[...], wo_ref[...], preferred_element_type=F32)
            y = (x_ref[...].astype(F32) + mixed).astype(BF16)
            acc[:, s * bn:(s + 1) * bn] = y.astype(F32)

    @pl.when(i == n_out)
    def _():
        n_rows, width = acc.shape
        cw = 1024

        def slab(r, _):
            rs = pl.ds(pl.multiple_of(r * 32, 32), 32)
            total = jnp.zeros((32, 128), F32)
            for c in range(0, width, cw):
                y = acc[rs, c:c + cw]
                sq = y * y
                for k in range(0, cw, 128):
                    total = total + sq[:, k:k + 128]
            inv = lax.rsqrt(jnp.sum(total, axis=-1, keepdims=True) / width + 1e-5)
            for c in range(0, width, cw):
                yn[rs, c:c + cw] = (acc[rs, c:c + cw] * inv * gm_ref[:, c:c + cw]).astype(BF16)
            return 0
        lax.fori_loop(0, n_rows // 32, slab, 0, unroll=2)

    @pl.when(i >= n_out)
    def _():
        gate = jnp.dot(yn[...], wg_ref[...], preferred_element_type=F32)
        up = jnp.dot(yn[...], wu_ref[...], preferred_element_type=F32)
        hidden = (gate * jax.nn.sigmoid(gate) * up).astype(BF16)
        width = acc.shape[1]
        step = width // 4
        for j in range(4):
            cs = slice(j * step, (j + 1) * step)
            acc[:, cs] += jnp.dot(hidden, wd_ref[:, cs], preferred_element_type=F32)

    @pl.when(i == n_out + n_ff - 1)
    def _():
        z_ref[...] = acc[...].astype(BF16)


def out_and_mlp(attn_rows, x_blk, w_out, g_mlp, w_gate, w_up, w_down):
    rows, width = x_blk.shape
    inner = attn_rows.shape[1]
    ff = w_gate.shape[1]
    bn = 512
    bf = 512
    n_out = width // bn
    n_ff = ff // bf
    one = pl.Buffered(1)
    c0 = lambda i: (0, 0)
    ffi = lambda i: jnp.maximum(i - n_out, 0)
    return pl.pallas_call(
        functools.partial(mlp_kernel, n_out, n_ff, bn),
        grid=(n_out + n_ff,),
        in_specs=[
            pl.BlockSpec((rows, inner), c0, pipeline_mode=one),
            pl.BlockSpec((rows, bn), lambda i: (0, jnp.minimum(i, n_out - 1))),
            pl.BlockSpec((inner, bn), lambda i: (0, jnp.minimum(i, n_out - 1))),
            pl.BlockSpec((1, width), c0, pipeline_mode=one),
            pl.BlockSpec((width, bf), lambda i: (0, ffi(i))),
            pl.BlockSpec((width, bf), lambda i: (0, ffi(i))),
            pl.BlockSpec((bf, width), lambda i: (ffi(i), 0)),
        ],
        out_specs=pl.BlockSpec((rows, width), c0, pipeline_mode=one),
        out_shape=jax.ShapeDtypeStruct((rows, width), BF16),
        scratch_shapes=[pltpu.VMEM((rows, width), F32), pltpu.VMEM((rows, width), BF16)],
        compiler_params=pltpu.CompilerParams(
            dimension_semantics=('arbitrary',), vmem_limit_bytes=VMEM_BYTES),
        name='out_mlp',
    )(attn_rows, x_blk, w_out, g_mlp.reshape(1, width), w_gate, w_up, w_down)


def solution(mesh):
    def local_layer(x_blk, g_attn, w_qkv, w_out, g_mlp, w_gate, w_up, w_down):
        n_heads, head_dim, model_width = w_out.shape
        attn_rows = attention(x_blk, g_attn, w_qkv, n_heads, head_dim)
        return out_and_mlp(attn_rows, x_blk, w_out.reshape(n_heads * head_dim, model_width), g_mlp, w_gate, w_up, w_down)

    row_spec = P(('data', 'seq'), None)
    return jax.shard_map(local_layer, mesh=mesh, in_specs=(row_spec, P(), P(), P(), P(), P(), P(), P()), out_specs=row_spec, check_vma=False)
```
